32 devices in a mesh: pair: 8 (over z, x), mp: 4 (over y, core).
Axes of the slice: x: 2, y: 2, z: 4, core: 2. Of those that a mesh axis runs over, the one named last changes fastest.
Arguments:
- current: bfloat16 [16, 196, 1024], P('pair'), may hold values from -6 to 6
- past_tokens: bfloat16 [16, 196, 1024], P('pair'), may hold values from -6 to 6
- counts: int32 [16], P('pair'), may hold values from 1 to 196, as said below
- partners: int32 [16], replicated, may hold values from 0 to 15, as said below
- query_weight: bfloat16 [1024, 1024], P(None, 'mp'), may hold values from -1.2 to 1.2
- key_weight: bfloat16 [1024, 1024], P(None, 'mp'), may hold values from -1.2 to 1.2
- value_weight: bfloat16 [1024, 1024], P(None, 'mp'), may hold values from -0.1875 to 0.1875
- output_weight: bfloat16 [1024, 1024], P('mp'), may hold values from -0.1875 to 0.1875
- up_weight: bfloat16 [1024, 4096], P(None, 'mp'), may hold values from -0.1875 to 0.1875
- down_weight: bfloat16 [4096, 1024], P('mp'), may hold values from -0.09375 to 0.09375
Outputs:
- decoded: bfloat16 [16, 196, 1024], P('pair', None, 'mp')
The draws below stay inside these ranges and needn't reach their ends.
Inputs may be any that keep to these rules, and one draw needn't show every extreme that they name: counts[p] is at most 196; some pair has exactly 196. A permutation of the pairs; partners[p] % 2 == p % 2; the partners of the 2 pairs of one pair index lie on distinct pair indices, and the pairs whose partners lie on one pair index come from distinct pair indices.
All inputs are finite; a program needn't handle non-finite values.
Results may differ from the reference program's by a relative error of at most 0.0085.
Values may be sent and summed in bfloat16 or wider, within the bound.
No kernel may reach another device: no remote copies, remote signals or barrier semaphores. Data moves between devices by JAX's collectives and lax.ppermute only.
A program may use at most 128 MiB of HBM per device.

```python
import jax
import jax.numpy as jnp
from jax import lax

D = 1024
HEADS = 16
HEAD_DIM = 64
FF = 4096
KEYS = 196
QSLOT = 196
PAIR_DEV = 2
PAIRS = 16


def pairing(key):
    groups = PAIRS // PAIR_DEV
    leading = jax.random.permutation(jax.random.fold_in(key, 11), groups)
    stride = 1 + jax.random.randint(jax.random.fold_in(key, 12), (), 0, max(groups // PAIR_DEV - 1, 1))
    positions = jnp.arange(PAIRS, dtype=jnp.int32)
    slot_of = positions % PAIR_DEV
    owner_of = positions // PAIR_DEV
    partner = (leading[owner_of] + slot_of * stride) % groups
    return (partner * PAIR_DEV + slot_of).astype(jnp.int32)


def past_rows(key):
    values = jnp.clip(jax.random.normal(jax.random.fold_in(key, 13), (PAIRS, KEYS, D), jnp.float32), -6.0, 6.0)
    return values


def query_key(key):
    common = jax.random.normal(jax.random.fold_in(key, 31), (D, D), jnp.float32)
    private = jax.random.normal(jax.random.fold_in(key, 32), (D, D), jnp.float32)
    query_part = common * D ** (-0.5)
    key_part = private * D ** (-0.5)
    return (jnp.clip(query_part, -1.2, 1.2), jnp.clip(key_part, -1.2, 1.2))


def draw_partners(key, part):
    return pairing(key)


def draw_past_tokens(key, part):
    return past_rows(key).astype(jnp.bfloat16)


def draw_current(key, part):
    values = jnp.clip(jax.random.normal(jax.random.fold_in(key, 21), (PAIRS, QSLOT, D), jnp.float32), -6.0, 6.0)
    return values.astype(jnp.bfloat16)


def draw_counts(key, part):
    drawn = jax.random.randint(jax.random.fold_in(key, 41), (PAIRS,), 0, KEYS)
    counts = KEYS - drawn * drawn // KEYS
    chosen = jax.random.randint(jax.random.fold_in(key, 42), (), 0, PAIRS)
    return jnp.where(jnp.arange(PAIRS, dtype=jnp.int32) == chosen, KEYS, counts).astype(jnp.int32)


def draw_query_weight(key, part):
    return query_key(key)[0].astype(jnp.bfloat16)


def draw_key_weight(key, part):
    return query_key(key)[1].astype(jnp.bfloat16)


def level_of(key, dims, cuts, least, top_value):
    loudness, own = 1.0, jax.random.fold_in(key, 6)
    for axis_at, parts in cuts:
        steps = jnp.exp(jax.random.uniform(jax.random.fold_in(own, axis_at), (parts,), jnp.float32, least / len(cuts), top_value / len(cuts)))
        loudness = loudness * jnp.repeat(steps, dims[axis_at] // parts).reshape([-1 if axis == axis_at else 1 for axis in range(len(dims))])
    return loudness


def bell_draw(rng, shape, width, limit, shards=(), held_as=jnp.bfloat16):
    values = width * jax.random.normal(rng, shape, jnp.float32)
    if shards:
        values = values * level_of(rng, shape, shards, -0.22, 0.18)
    return jnp.clip(values, -limit, limit).astype(held_as)


def setup_inputs(seed: int = 0) -> dict:
    key_of = jax.random.split(jax.random.key(seed), 11)
    current = draw_current(jax.random.fold_in(key_of[10], 71), 0)
    past_tokens = draw_past_tokens(jax.random.fold_in(key_of[10], 71), 0)
    counts = draw_counts(jax.random.fold_in(key_of[10], 71), 0)
    partners = draw_partners(jax.random.fold_in(key_of[10], 71), 0)
    query_weight = draw_query_weight(jax.random.fold_in(key_of[10], 71), 0)
    key_weight = draw_key_weight(jax.random.fold_in(key_of[10], 71), 0)
    value_weight = bell_draw(key_of[6], (D, D), D ** -0.5, 0.1875, ((1, 4),))
    output_weight = bell_draw(key_of[7], (D, D), D ** -0.5, 0.1875, ((0, 4),))
    up_weight = bell_draw(key_of[8], (D, FF), D ** -0.5, 0.1875, ((1, 4),))
    down_weight = bell_draw(key_of[9], (FF, D), FF ** -0.5, 0.09375, ((0, 4),))
    return dict(current=current, past_tokens=past_tokens, counts=counts, partners=partners, query_weight=query_weight, key_weight=key_weight, value_weight=value_weight, output_weight=output_weight, up_weight=up_weight, down_weight=down_weight)


def layer_norm(values):
    center = values - lax.optimization_barrier(jnp.mean(values, axis=-1, keepdims=True))
    spread = lax.optimization_barrier(jnp.mean(center * center, axis=-1, keepdims=True))
    return center * lax.rsqrt(spread + 1e-06)

def attend(inputs):
    query_block, key_block, value_block = inputs
    scores = jnp.einsum('qhd,khd->hqk', query_block.astype(jnp.float32), key_block.astype(jnp.float32)) * HEAD_DIM ** (-0.5)
    row_max = lax.optimization_barrier(jnp.max(scores, axis=-1, keepdims=True))
    lifted = jnp.exp(scores - row_max)
    weights = (lifted / lax.optimization_barrier(jnp.sum(lifted, axis=-1, keepdims=True))).astype(jnp.bfloat16)
    return jnp.einsum('hqk,khd->qhd', weights.astype(jnp.float32), value_block.astype(jnp.float32)).astype(jnp.bfloat16)

def reference(current, past_tokens, counts, partners, query_weight, key_weight, value_weight, output_weight, up_weight, down_weight):
    model_width = current.shape[2]
    normed = layer_norm(current.astype(jnp.float32)).astype(jnp.bfloat16).reshape(-1, model_width)
    context = layer_norm(past_tokens.astype(jnp.float32)).astype(jnp.bfloat16).reshape(-1, model_width)
    queries = jnp.dot(normed, query_weight, preferred_element_type=jnp.float32).astype(jnp.bfloat16).reshape(PAIRS, QSLOT, HEADS, HEAD_DIM)
    keys_all = jnp.dot(context, key_weight, preferred_element_type=jnp.float32).astype(jnp.bfloat16).reshape(PAIRS, KEYS, HEADS, HEAD_DIM)
    values_all = jnp.dot(context, value_weight, preferred_element_type=jnp.float32).astype(jnp.bfloat16).reshape(PAIRS, KEYS, HEADS, HEAD_DIM)
    attended = lax.map(attend, (queries, keys_all[partners], values_all[partners]))
    projected = jnp.dot(attended.reshape(-1, model_width), output_weight, preferred_element_type=jnp.float32)
    hidden = current.astype(jnp.float32).reshape(-1, model_width) + projected
    mixer_in = layer_norm(hidden).astype(jnp.bfloat16)
    expanded = jax.nn.gelu(jnp.dot(mixer_in, up_weight, preferred_element_type=jnp.float32), approximate=False).astype(jnp.bfloat16)
    result = hidden + jnp.dot(expanded, down_weight, preferred_element_type=jnp.float32)
    is_live = (jnp.arange(QSLOT, dtype=jnp.int32)[None, :] < counts[:, None]).reshape(-1, 1)
    result = jnp.where(is_live, result, 0.0)
    return result.reshape(PAIRS, QSLOT, model_width).astype(jnp.bfloat16)
```

```python
import jax
import jax.numpy as jnp
from jax import lax
from jax.experimental import pallas as pl
from jax.experimental.pallas import tpu as pltpu
from jax.sharding import PartitionSpec as P

HEAD_DIM = 64
F32, BF16 = jnp.float32, jnp.bfloat16
VMEM = pl.BlockSpec(memory_space=pltpu.VMEM)
SMEM = pl.BlockSpec(memory_space=pltpu.SMEM)


def layer_norm(values):
    center = values - jnp.mean(values, axis=-1, keepdims=True)
    spread = jnp.mean(center * center, axis=-1, keepdims=True)
    return center * lax.rsqrt(spread + 1e-06)


def erf_gelu(v):
    return 0.5 * v * (1.0 + lax.erf(v * (0.5**0.5)))


def mm(a, b):
    return jnp.dot(a, b, preferred_element_type=F32)


def call(kernel, outs, ins, flops, limit=16 << 20, scratch=(), name=None):
    specs = [SMEM if a.dtype == jnp.int32 else VMEM for a in ins]
    moved = sum(a.size * a.dtype.itemsize for a in list(ins) + list(outs))
    return pl.pallas_call(
        kernel,
        out_shape=list(outs),
        in_specs=specs,
        out_specs=[VMEM] * len(outs),
        scratch_shapes=list(scratch),
        name=name,
        cost_estimate=pl.CostEstimate(flops=flops, bytes_accessed=moved, transcendentals=0),
        compiler_params=pltpu.CompilerParams(vmem_limit_bytes=limit),
    )(*ins)


def struct(shape, dtype=BF16):
    return jax.ShapeDtypeStruct(shape, dtype)


def source_slot(partners, dest, mine, pair_count):
    slot = 0
    for j in range(pair_count):
        q = partners[dest * pair_count + j]
        slot = jnp.where(lax.div(q, pair_count) == mine, lax.rem(q, pair_count), slot)
    return slot


def pack_kernel(groups, partners, past, *refs):
    outs, normed = refs[:-1], refs[-1]
    pair_count = past.shape[1]
    width = outs[0].shape[-1]
    for p in range(pair_count):
        normed[p] = layer_norm(past[:, p, :].astype(F32)).astype(BF16)
    mine = lax.axis_index("pair")
    start = pl.multiple_of(lax.axis_index("mp") * width, width)
    for k in range(groups):
        slot = source_slot(partners, lax.rem(mine + k, groups), mine, pair_count)
        outs[k][...] = normed[slot, :, pl.ds(start, width)]


def query_kernel(current, weight, queries):
    for p in range(current.shape[1]):
        normed = layer_norm(current[:, p, :].astype(F32)).astype(BF16)
        queries[p] = mm(normed, weight[...]).astype(BF16)


def select_kernel(groups, partners, *refs):
    incoming, out = refs[:-1], refs[-1]
    pair_count = out.shape[0]
    mine = lax.axis_index("pair")
    for j in range(pair_count):
        owner = lax.div(partners[mine * pair_count + j], pair_count)
        shift = lax.rem(mine - owner + groups, groups)
        for k in range(groups):

            @pl.when(shift == k)
            def _():
                out[j] = incoming[k][...]


def attend_kernel(shards, queries, key_weight, value_weight, *refs):
    context, out = refs[:-1], refs[-1]
    pair_count, slot_count, features = queries.shape
    heads = features // HEAD_DIM
    width = context[0].shape[-1]
    me = lax.axis_index("mp")
    lane_head = lax.broadcasted_iota(jnp.int32, (1, features), 1) // HEAD_DIM
    for p in range(pair_count):
        keys = values = 0.0
        for k in range(shards):
            rows = pl.ds(pl.multiple_of((me ^ k) * width, width), width)
            keys += mm(context[k][p], key_weight[rows, :])
            values += mm(context[k][p], value_weight[rows, :])
        keys, values = keys.astype(BF16), values.astype(BF16)
        asked = queries[p]
        total = jnp.zeros((slot_count, features), F32)
        for h in range(heads):
            mask = lane_head == h
            scores = lax.dot_general(
                jnp.where(mask, asked, jnp.zeros_like(asked)),
                keys,
                (((1,), (1,)), ((), ())),
                preferred_element_type=F32,
            )
            scores = scores * HEAD_DIM ** (-0.5)
            lifted = jnp.exp(scores - jnp.max(scores, axis=-1, keepdims=True))
            weights = lifted * (1.0 / jnp.sum(lifted, axis=-1, keepdims=True))
            total = jnp.where(mask, mm(weights.astype(BF16), values), total)
        out[p] = total.astype(BF16)


def columns(k, width):
    return pl.ds(pl.multiple_of((lax.axis_index("mp") ^ k) * width, width), width)


def mixer_kernel(shards, away, current, up, down, *refs):
    attended, output_weight = refs[:shards], refs[shards : 2 * shards]
    expanded, share = refs[2 * shards : 2 * shards + 2]
    sent = refs[2 * shards + 2 : -1]
    hold = refs[-1]
    width = share.shape[-1]
    for p in range(current.shape[1]):
        hidden = current[:, p, :].astype(F32)
        for k in range(shards):
            hidden += mm(attended[k][p], output_weight[k][...])
        hold[...] = hidden
        share[p] = hold[:, columns(0, width)]
        mixer_in = layer_norm(hidden).astype(BF16)
        expanded[p] = erf_gelu(mm(mixer_in, up[...])).astype(BF16)
        for k, out in zip(away, sent):
            out[p] = mm(expanded[p], down[:, columns(k, width)]).astype(BF16)


def near_kernel(near, expanded, share, down, *refs):
    width = share.shape[-1]
    for p in range(share.shape[0]):
        for k, out in zip(near, refs):
            part = mm(expanded[p], down[:, columns(k, width)])
            out[p] = share[p] + part if k == 0 else part.astype(BF16)


def add_kernel(left, right, out):
    out[...] = (left[...].astype(F32) + right[...].astype(F32)).astype(BF16)


def final_kernel(counts, base, *refs):
    parts, out = refs[:-1], refs[-1]
    for p in range(base.shape[0]):
        total = base[p]
        for part in parts:
            total += part[p].astype(F32)
        live = lax.broadcasted_iota(jnp.int32, (total.shape[0], 1), 0) < counts[p]
        out[:, p, :] = jnp.where(live, total, 0.0).astype(BF16)


def swap(value, stride):
    size = lax.axis_size("mp")
    return lax.ppermute(value, "mp", [(i, i ^ stride) for i in range(size)])


def gather(block):
    size = lax.axis_size("mp")
    blocks, stride = {0: block}, size // 2
    while stride:
        blocks |= {k ^ stride: swap(v, stride) for k, v in blocks.items()}
        stride //= 2
    return [blocks[k] for k in range(size)]


def exchange(entries):
    groups = lax.axis_size("pair")
    if groups <= 8:
        return [entries[0]] + [
            lax.ppermute(entries[k], "pair", [(i, (i + k) % groups) for i in range(groups)])
            for k in range(1, groups)
        ]
    mine = lax.axis_index("pair")
    order = (jnp.arange(groups) - mine) % groups
    moved = lax.all_to_all(jnp.stack(entries)[order], "pair", 0, 0, tiled=True)
    moved = moved[(mine - jnp.arange(groups)) % groups]
    return [moved[k] for k in range(groups)]


def body(
    current,
    past_tokens,
    counts,
    partners,
    query_weight,
    key_weight,
    value_weight,
    output_weight,
    up_weight,
    down_weight,
):
    pair_count, slot_count, model_width = current.shape
    key_count = past_tokens.shape[1]
    features = query_weight.shape[1]
    groups, shards = lax.axis_size("pair"), lax.axis_size("mp")
    width = model_width // shards
    rows = pair_count * slot_count
    hidden_units = up_weight.shape[1]
    current_rows = current.transpose(1, 0, 2)
    past_rows = past_tokens.transpose(1, 0, 2)

    def part(fn, *static):
        return lambda *refs: fn(*static, *refs)

    entries = call(
        part(pack_kernel, groups),
        [struct((key_count, width))] * groups,
        [partners, past_rows],
        flops=rows * model_width * 10,
        scratch=[pltpu.VMEM((pair_count, key_count, model_width), BF16)],
        name="pack",
    )
    incoming = exchange(entries)
    (queries,) = call(
        query_kernel,
        [struct((pair_count, slot_count, features))],
        [current_rows, query_weight],
        flops=2 * rows * model_width * features,
        name="query",
    )
    output_weights = gather(output_weight)
    (wanted,) = call(
        part(select_kernel, groups),
        [struct((pair_count, key_count, width))],
        [partners, *incoming],
        flops=rows * width,
        name="select",
    )
    context = gather(wanted)
    (attended,) = call(
        part(attend_kernel, shards),
        [struct((pair_count, slot_count, features))],
        [queries, key_weight, value_weight, *context],
        flops=4 * rows * model_width * features,
        name="attend",
    )
    attended = gather(attended)
    away, near = range(shards - 1, shards // 2 - 1, -1), range(shards // 2 - 1, -1, -1)
    block = struct((pair_count, slot_count, width))
    expanded, share, *sums = call(
        part(mixer_kernel, shards, away),
        [
            struct((pair_count, slot_count, hidden_units)),
            struct((pair_count, slot_count, width), F32),
            *[block] * len(away),
        ],
        [current_rows, up_weight, down_weight, *attended, *output_weights],
        flops=5 * rows * model_width * hidden_units,
        scratch=[pltpu.VMEM((slot_count, model_width), F32)],
        limit=24 << 20,
        name="mixer",
    )
    partial = dict(zip(away, sums))
    near_parts = call(
        part(near_kernel, near),
        [*[block] * (len(near) - 1), struct((pair_count, slot_count, width), F32)],
        [expanded, share, down_weight],
        flops=rows * model_width * hidden_units,
        name="near",
    )
    partial |= dict(zip(near, near_parts))

    def fold(part_of):
        part_of, stride = dict(part_of), 1
        while stride < shards // 2:
            for k in [k for k in part_of if k & stride]:
                received = swap(part_of.pop(k), stride)
                yield k ^ stride, received, part_of
            stride *= 2

    far = {k: partial[k] for k in away}
    for k, received, far in fold(far):
        (far[k],) = call(add_kernel, [block], [far[k], received], flops=rows * width, name="add")
    crossed = swap(far[shards // 2], shards // 2)
    close = {k: partial[k] for k in near if k}
    terms, stride = [], 1
    close[0] = None
    while stride < shards // 2:
        for k in [k for k in close if k & stride]:
            received = swap(close.pop(k), stride)
            if k ^ stride:
                (close[k ^ stride],) = call(
                    add_kernel, [block], [close[k ^ stride], received], flops=rows * width, name="add"
                )
            else:
                terms.append(received)
        stride *= 2
    (result,) = call(
        final_kernel,
        [struct((slot_count, pair_count, width))],
        [counts, partial[0], *terms, crossed],
        flops=rows * width,
        name="final",
    )
    return result.transpose(1, 0, 2)


def solution(mesh):
    placed = (
        P("pair", None, None),
        P("pair", None, None),
        P("pair"),
        P(),
        P(None, "mp"),
        P(None, "mp"),
        P(None, "mp"),
        P("mp", None),
        P(None, "mp"),
        P("mp", None),
    )
    return jax.shard_map(
        body, mesh=mesh, in_specs=placed, out_specs=P("pair", None, "mp"), check_vma=False
    )
```

```python
import jax
import jax.numpy as jnp
from jax import lax
from jax.experimental import pallas as pl
from jax.experimental.pallas import tpu as pltpu
from jax.sharding import PartitionSpec as P


HEAD_DIM = 64
F32, BF16 = jnp.float32, jnp.bfloat16
VMEM = pl.BlockSpec(memory_space=pltpu.VMEM)
SMEM = pl.BlockSpec(memory_space=pltpu.SMEM)
HBM = pl.BlockSpec(memory_space=pltpu.HBM)


def layer_norm(values):
    center = values - jnp.mean(values, axis=-1, keepdims=True)
    spread = jnp.mean(center * center, axis=-1, keepdims=True)
    return center * lax.rsqrt(spread + 1e-06)


def erf_gelu(v):
    return 0.5 * v * (1.0 + lax.erf(v * (0.5**0.5)))


def mm(a, b):
    return jnp.dot(a, b, preferred_element_type=F32)


def call(kernel, outs, ins, flops, limit=16 << 20, scratch=(), specs=None):
    specs = specs or [SMEM if a.dtype == jnp.int32 else VMEM for a in ins]
    moved = sum(a.size * a.dtype.itemsize for a in list(ins) + list(outs))
    return pl.pallas_call(
        kernel,
        out_shape=list(outs),
        in_specs=specs,
        out_specs=[VMEM] * len(outs),
        scratch_shapes=list(scratch),
        cost_estimate=pl.CostEstimate(flops=flops, bytes_accessed=moved, transcendentals=0),
        compiler_params=pltpu.CompilerParams(vmem_limit_bytes=limit),
    )(*ins)


def struct(shape, dtype=BF16):
    return jax.ShapeDtypeStruct(shape, dtype)


def source_slot(partners, dest, mine, pair_count):
    slot = 0
    for j in range(pair_count):
        q = partners[dest * pair_count + j]
        slot = jnp.where(lax.div(q, pair_count) == mine, lax.rem(q, pair_count), slot)
    return slot


def pack_kernel(groups, partners_hbm, past, *refs):
    outs = refs[:groups]
    partners, rows, halves, sems = refs[groups:]
    pair_count = past.shape[1]
    width = outs[0].shape[-1]
    mine = lax.axis_index("pair")
    start = pl.multiple_of(lax.axis_index("mp") * width, width)
    table = pltpu.make_async_copy(partners_hbm, partners, sems.at[0])
    block = pltpu.make_async_copy(past.at[:, :, pl.ds(start, width)], rows, sems.at[1])
    block.start()
    table.start()
    table.wait()
    block.wait()
    for p in range(pair_count):
        halves[p] = rows[:, p, :].astype(F32).astype(BF16)
    for k in range(groups):
        slot = source_slot(partners, lax.rem(mine + k, groups), mine, pair_count)
        outs[k][...] = halves[slot]


def query_kernel(current, weight, *refs):
    held = len(refs) // 2
    queries = refs[held]
    for p in range(current.shape[1]):
        normed = layer_norm(current[:, p, :].astype(F32)).astype(BF16)
        queries[p] = mm(normed, weight[...]).astype(BF16)
    for source, kept in zip(refs[:held], refs[held + 1 :]):
        kept[...] = source[...]


def select_kernel(groups, partners, *refs):
    incoming, outs = refs[:groups], refs[groups + 1 :]
    pair_count = len(outs)
    mine = lax.axis_index("pair")
    for p, out in enumerate(outs):
        owner = lax.div(partners[mine * pair_count + p], pair_count)
        shift = lax.rem(mine - owner + groups, groups)
        for k in range(groups):

            @pl.when(shift == k)
            def _():
                out[...] = incoming[k][...]


def attend_kernel(shards, pair, queries, key_weight, value_weight, *refs):
    context, out = refs[:-1], refs[-1]
    slot_count, features = out.shape
    width = context[0].shape[-1]
    me = lax.axis_index("mp")
    lane_head = lax.broadcasted_iota(jnp.int32, (1, features), 1) // HEAD_DIM
    scale = 1.0 / (shards * width)
    blocks = [block[...].astype(F32) for block in context]
    mean = sum(jnp.sum(v, axis=-1, keepdims=True) for v in blocks) * scale
    blocks = [v - mean for v in blocks]
    spread = sum(jnp.sum(v * v, axis=-1, keepdims=True) for v in blocks) * scale
    factor = lax.rsqrt(spread + 1e-06)
    keys = values = 0.0
    for k in range(shards):
        normed = (blocks[k] * factor).astype(BF16)
        rows = pl.ds(pl.multiple_of((me ^ k) * width, width), width)
        keys += mm(normed, key_weight[rows, :])
        values += mm(normed, value_weight[rows, :])
    keys, values = keys.astype(BF16), values.astype(BF16)
    asked = queries[pair]
    total = jnp.zeros((slot_count, features), F32)
    for h in range(features // HEAD_DIM):
        mask = lane_head == h
        scores = lax.dot_general(
            jnp.where(mask, asked, jnp.zeros_like(asked)),
            keys,
            (((1,), (1,)), ((), ())),
            preferred_element_type=F32,
        )
        scores = scores * HEAD_DIM ** (-0.5)
        lifted = jnp.exp(scores - jnp.max(scores, axis=-1, keepdims=True))
        weights = lifted * (1.0 / jnp.sum(lifted, axis=-1, keepdims=True))
        total = jnp.where(mask, mm(weights.astype(BF16), values), total)
    out[...] = total.astype(BF16)


def columns(k, width):
    return pl.ds(pl.multiple_of((lax.axis_index("mp") ^ k) * width, width), width)


def mixer_kernel(shards, away, pair, current, up, down, *refs):
    attended, output_weight = refs[:shards], refs[shards : 2 * shards]
    expanded, share = refs[2 * shards : 2 * shards + 2]
    sent = refs[2 * shards + 2 : -1]
    hold = refs[-1]
    width = share.shape[-1]
    hidden = current[:, pair, :].astype(F32)
    for k in range(shards):
        hidden += mm(attended[k][...], output_weight[k][...])
    hold[...] = hidden
    share[...] = hold[:, columns(0, width)]
    mixer_in = layer_norm(hidden).astype(BF16)
    expanded[...] = erf_gelu(mm(mixer_in, up[...])).astype(BF16)
    for k, out in zip(away, sent):
        out[...] = mm(expanded[...], down[:, columns(k, width)]).astype(BF16)


def near_kernel(near, expanded, share, down, *refs):
    width = share.shape[-1]
    for k, out in zip(near, refs):
        part = mm(expanded[...], down[:, columns(k, width)])
        out[...] = share[...] + part if k == 0 else part.astype(BF16)


def add_kernel(left, right, out):
    out[...] = (left[...].astype(F32) + right[...].astype(F32)).astype(BF16)


def final_kernel(pair_count, counts, *refs):
    terms, out, hold = refs[:-2], refs[-2], refs[-1]
    slot_count, width = terms[0].shape
    lanes = hold.shape[-1]
    each = len(terms) // pair_count
    for p in range(pair_count):
        total = sum(term[...].astype(F32) for term in terms[p * each : (p + 1) * each])
        live = lax.broadcasted_iota(jnp.int32, (slot_count, 1), 0) < counts[p]
        total = jnp.where(live, total, 0.0)
        for j in range(width // lanes):
            hold[j, pl.ds(p, slot_count, stride=pair_count), :] = total[:, j * lanes : (j + 1) * lanes]
    for j in range(width // lanes):
        tile = hold[j].reshape(slot_count, pair_count, lanes).astype(BF16)
        out[:, :, j * lanes : (j + 1) * lanes] = tile


def swap(value, stride):
    size = lax.axis_size("mp")
    return lax.ppermute(value, "mp", [(i, i ^ stride) for i in range(size)])


def gather(block):
    size = lax.axis_size("mp")
    blocks, stride = {0: block}, size // 2
    while stride:
        blocks |= {k ^ stride: swap(v, stride) for k, v in blocks.items()}
        stride //= 2
    return [blocks[k] for k in range(size)]


def exchange(entries):
    groups = lax.axis_size("pair")
    if groups <= 8:
        moved = [entries[0]]
        for k in range(1, groups):
            ring = [(i, (i + k) % groups) for i in range(groups)]
            moved.append(lax.ppermute(entries[k], "pair", ring))
        return moved
    mine = lax.axis_index("pair")
    order = (jnp.arange(groups) - mine) % groups
    moved = lax.all_to_all(jnp.stack(entries)[order], "pair", 0, 0, tiled=True)
    moved = moved[(mine - jnp.arange(groups)) % groups]
    return [moved[k] for k in range(groups)]


def body(
    current,
    past_tokens,
    counts,
    partners,
    query_weight,
    key_weight,
    value_weight,
    output_weight,
    up_weight,
    down_weight,
):
    pair_count, slot_count, model_width = current.shape
    key_count = past_tokens.shape[1]
    features = query_weight.shape[1]
    groups, shards = lax.axis_size("pair"), lax.axis_size("mp")
    width = model_width // shards
    rows = pair_count * slot_count
    hidden_units = up_weight.shape[1]
    query_shape = struct((pair_count, slot_count, features))
    current_rows = current.transpose(1, 0, 2)
    past_rows = past_tokens.transpose(1, 0, 2)

    def part(fn, *static):
        return lambda *refs: fn(*static, *refs)

    entries = call(
        part(pack_kernel, groups),
        [struct((key_count, width))] * groups,
        [partners, past_rows],
        flops=rows * width,
        scratch=[
            pltpu.SMEM(partners.shape, jnp.int32),
            pltpu.VMEM((key_count, pair_count, width), BF16),
            pltpu.VMEM((pair_count, key_count, width), BF16),
            pltpu.SemaphoreType.DMA((2,)),
        ],
        specs=[HBM, HBM],
        limit=63 << 20,
    )
    incoming = exchange(entries)
    output_weights = gather(output_weight)
    queries, key_weight, value_weight, output_weights[0] = call(
        query_kernel,
        [struct(a.shape) for a in (query_shape, key_weight, value_weight, output_weight)],
        [current_rows, query_weight, key_weight, value_weight, output_weight],
        flops=2 * rows * model_width * features,
    )
    away, near = range(shards - 1, shards // 2 - 1, -1), range(shards // 2 - 1, -1, -1)
    block = struct((slot_count, width))
    wide = struct((slot_count, width), F32)

    def narrow(part_of):
        stride, alone = 1, []
        while stride < shards // 2:
            for k in [k for k in part_of if k & stride]:
                received = swap(part_of.pop(k), stride)
                if k ^ stride:
                    (part_of[k ^ stride],) = call(
                        add_kernel,
                        [block],
                        [part_of[k ^ stride], received],
                        flops=slot_count * width,
                    )
                else:
                    alone.append(received)
            stride *= 2
        return alone

    context, attended, terms = [], [], []
    wanted = call(
        part(select_kernel, groups),
        [struct((key_count, width))] * pair_count,
        [partners, *incoming, queries],
        flops=rows * width,
        specs=[SMEM, *[VMEM] * groups, pl.BlockSpec(memory_space=pl.ANY)],
    )
    for p in range(pair_count):
        context.append(gather(wanted[p]))
    for p in range(pair_count):
        (done,) = call(
            part(attend_kernel, shards, p),
            [struct((slot_count, features))],
            [queries, key_weight, value_weight, *context[p]],
            flops=4 * rows // pair_count * model_width * features,
        )
        attended.append(gather(done))
    for p in range(pair_count):
        expanded, share, *sums = call(
            part(mixer_kernel, shards, away, p),
            [struct((slot_count, hidden_units)), wide, *[block] * len(away)],
            [current_rows, up_weight, down_weight, *attended[p], *output_weights],
            flops=5 * slot_count * model_width * hidden_units,
            scratch=[pltpu.VMEM((slot_count, model_width), F32)],
            limit=24 << 20,
        )
        far = dict(zip(away, sums))
        narrow(far)
        crossed = swap(far[shards // 2], shards // 2)
        close = dict(
            zip(
                near,
                call(
                    part(near_kernel, near),
                    [*[block] * (len(near) - 1), wide],
                    [expanded, share, down_weight],
                    flops=slot_count * model_width * hidden_units,
                ),
            )
        )
        base = close.pop(0)
        terms += [base, *narrow(close), crossed]
    (result,) = call(
        part(final_kernel, pair_count),
        [struct((slot_count, pair_count, width))],
        [counts, *terms],
        flops=rows * width,
        scratch=[pltpu.VMEM((width // 128, rows, 128), F32)],
    )
    return result.transpose(1, 0, 2)


def solution(mesh):
    placed = (
        P("pair", None, None),
        P("pair", None, None),
        P("pair"),
        P(),
        P(None, "mp"),
        P(None, "mp"),
        P(None, "mp"),
        P("mp", None),
        P(None, "mp"),
        P("mp", None),
    )

    return jax.shard_map(
        body, mesh=mesh, in_specs=placed, out_specs=P("pair", None, "mp"), check_vma=False
    )
```

```python
import jax
import jax.numpy as jnp
from jax import lax
from jax.experimental import pallas as pl
from jax.experimental.pallas import tpu as pltpu
from jax.sharding import PartitionSpec as P


HEAD_DIM = 64
F32, BF16 = jnp.float32, jnp.bfloat16
VMEM = pl.BlockSpec(memory_space=pltpu.VMEM)
SMEM = pl.BlockSpec(memory_space=pltpu.SMEM)
HBM = pl.BlockSpec(memory_space=pltpu.HBM)


def layer_norm(values):
    center = values - jnp.mean(values, axis=-1, keepdims=True)
    spread = jnp.mean(center * center, axis=-1, keepdims=True)
    return center * lax.rsqrt(spread + 1e-06)


def erf_gelu(v):
    return 0.5 * v * (1.0 + lax.erf(v * (0.5**0.5)))


def mm(a, b):
    return jnp.dot(a, b, preferred_element_type=F32)


def call(kernel, outs, ins, flops, limit=16 << 20, scratch=(), specs=None):
    specs = specs or [SMEM if a.dtype == jnp.int32 else VMEM for a in ins]
    moved = sum(a.size * a.dtype.itemsize for a in list(ins) + list(outs))
    return pl.pallas_call(
        kernel,
        out_shape=list(outs),
        in_specs=specs,
        out_specs=[VMEM] * len(outs),
        scratch_shapes=list(scratch),
        cost_estimate=pl.CostEstimate(flops=flops, bytes_accessed=moved, transcendentals=0),
        compiler_params=pltpu.CompilerParams(vmem_limit_bytes=limit),
    )(*ins)


def struct(shape, dtype=BF16):
    return jax.ShapeDtypeStruct(shape, dtype)


def wrap(index, size):
    return jnp.where(index >= size, index - size, index)


def source_slot(partners, dest, mine, pair_count):
    slot = 0
    for j in range(pair_count):
        near = partners[dest * pair_count + j] - mine * pair_count
        slot = jnp.where((near >= 0) & (near < pair_count), near, slot)
    return slot


def pack_kernel(groups, partners_hbm, past, *refs):
    outs, shifts = refs[:groups], refs[groups]
    partners, rows, halves, sems = refs[groups + 1 :]
    pair_count = past.shape[1]
    width = outs[0].shape[-1]
    mine = lax.axis_index("pair")
    start = pl.multiple_of(lax.axis_index("mp") * width, width)
    table = pltpu.make_async_copy(partners_hbm, partners, sems.at[0])
    block = pltpu.make_async_copy(past.at[:, :, pl.ds(start, width)], rows, sems.at[1])
    block.start()
    table.start()
    table.wait()
    slots = [source_slot(partners, wrap(mine + k, groups), mine, pair_count) for k in range(groups)]
    for p in range(pair_count):
        wanted, shift = partners[mine * pair_count + p], 0
        for k in range(1, groups):
            near = wanted - wrap(mine + groups - k, groups) * pair_count
            shift = jnp.where((near >= 0) & (near < pair_count), k, shift)
        shifts[pl.ds(p, 1), :] = jnp.full((1, shifts.shape[1]), shift, jnp.int32).astype(F32)
    block.wait()
    for p in range(pair_count):
        halves[p] = rows[:, p, :].astype(F32).astype(BF16)
    for k in range(groups):
        outs[k][...] = halves[slots[k]]


def query_kernel(current, weight, queries):
    for p in range(current.shape[1]):
        normed = layer_norm(current[:, p, :].astype(F32)).astype(BF16)
        queries[p] = mm(normed, weight[...]).astype(BF16)


def stage_kernel(*refs):
    held = len(refs) // 2
    for source, kept in zip(refs[:held], refs[held:]):
        kept[...] = source[...]


def select_kernel(groups, table, *refs):
    incoming, outs = refs[:groups], refs[groups:]
    for p, out in enumerate(outs):
        shift = jnp.max(table[pl.ds(p, 1), :])
        for k in range(groups):

            @pl.when(shift == float(k))
            def _():
                out[...] = incoming[k][...]


def attend_kernel(shards, pair, queries, key_weight, value_weight, *refs):
    context, out = refs[:-1], refs[-1]
    slot_count, features = out.shape
    width = context[0].shape[-1]
    me = lax.axis_index("mp")
    lane_head = lax.broadcasted_iota(jnp.int32, (1, features), 1) // HEAD_DIM
    scale = 1.0 / (shards * width)
    blocks = [block[...].astype(F32) for block in context]
    mean = sum(jnp.sum(v, axis=-1, keepdims=True) for v in blocks) * scale
    blocks = [v - mean for v in blocks]
    spread = sum(jnp.sum(v * v, axis=-1, keepdims=True) for v in blocks) * scale
    factor = lax.rsqrt(spread + 1e-06)
    keys = values = 0.0
    for k in range(shards):
        normed = (blocks[k] * factor).astype(BF16)
        rows = pl.ds(pl.multiple_of((me ^ k) * width, width), width)
        keys += mm(normed, key_weight[rows, :])
        values += mm(normed, value_weight[rows, :])
    keys, values = keys.astype(BF16), values.astype(BF16)
    asked = queries[pair]
    total = jnp.zeros((slot_count, features), F32)
    for h in range(features // HEAD_DIM):
        mask = lane_head == h
        scores = lax.dot_general(
            jnp.where(mask, asked, jnp.zeros_like(asked)),
            keys,
            (((1,), (1,)), ((), ())),
            preferred_element_type=F32,
        )
        scores = scores * HEAD_DIM ** (-0.5)
        lifted = jnp.exp(scores - jnp.max(scores, axis=-1, keepdims=True))
        weights = lifted * (1.0 / jnp.sum(lifted, axis=-1, keepdims=True))
        total = jnp.where(mask, mm(weights.astype(BF16), values), total)
    out[...] = total.astype(BF16)


def columns(k, width):
    return pl.ds(pl.multiple_of((lax.axis_index("mp") ^ k) * width, width), width)


def early_kernel(pair, current, *refs):
    count = (len(refs) - 1) // 2
    hidden = current[:, pair, :].astype(F32)
    for attended, weight in zip(refs[:count], refs[count:-1]):
        hidden += mm(attended[...], weight[...])
    refs[-1][...] = hidden


def mixer_kernel(away, early, attended, output_weight, up, down, expanded, share, *refs):
    sent, hold = refs[:-1], refs[-1]
    width = share.shape[-1]
    hidden = early[...] + mm(attended[...], output_weight[...])
    hold[...] = hidden
    share[...] = hold[:, columns(0, width)]
    mixer_in = layer_norm(hidden).astype(BF16)
    expanded[...] = erf_gelu(mm(mixer_in, up[...])).astype(BF16)
    for k, out in zip(away, sent):
        out[...] = mm(expanded[...], down[:, columns(k, width)]).astype(BF16)


def near_kernel(near, expanded, share, down, *refs):
    width = share.shape[-1]
    for k, out in zip(near, refs):
        part = mm(expanded[...], down[:, columns(k, width)])
        out[...] = share[...] + part if k == 0 else part.astype(BF16)


def add_kernel(left, right, out):
    out[...] = (left[...].astype(F32) + right[...].astype(F32)).astype(BF16)


def final_kernel(pair_count, counts, *refs):
    terms, out, hold = refs[:-2], refs[-2], refs[-1]
    slot_count, width = terms[0].shape
    lanes = hold.shape[-1]
    each = len(terms) // pair_count
    for p in range(pair_count):
        total = sum(term[...].astype(F32) for term in terms[p * each : (p + 1) * each])
        live = lax.broadcasted_iota(jnp.int32, (slot_count, 1), 0) < counts[p]
        total = jnp.where(live, total, 0.0)
        for j in range(width // lanes):
            hold[j, pl.ds(p, slot_count, stride=pair_count), :] = total[:, j * lanes : (j + 1) * lanes]
    for j in range(width // lanes):
        tile = hold[j].reshape(slot_count, pair_count, lanes).astype(BF16)
        out[:, :, j * lanes : (j + 1) * lanes] = tile


def swap(value, stride):
    size = lax.axis_size("mp")
    return lax.ppermute(value, "mp", [(i, i ^ stride) for i in range(size)])


def gather(block):
    size = lax.axis_size("mp")
    blocks, stride = {0: block}, size // 2
    while stride:
        blocks |= {k ^ stride: swap(v, stride) for k, v in blocks.items()}
        stride //= 2
    return [blocks[k] for k in range(size)]


def exchange(entries):
    groups = lax.axis_size("pair")
    if groups <= 8:
        moved = [entries[0]]
        for k in range(1, groups):
            ring = [(i, (i + k) % groups) for i in range(groups)]
            moved.append(lax.ppermute(entries[k], "pair", ring))
        return moved
    mine = lax.axis_index("pair")
    order = (jnp.arange(groups) - mine) % groups
    moved = lax.all_to_all(jnp.stack(entries)[order], "pair", 0, 0, tiled=True)
    moved = moved[(mine - jnp.arange(groups)) % groups]
    return [moved[k] for k in range(groups)]


def body(
    current,
    past_tokens,
    counts,
    partners,
    query_weight,
    key_weight,
    value_weight,
    output_weight,
    up_weight,
    down_weight,
):
    pair_count, slot_count, model_width = current.shape
    key_count = past_tokens.shape[1]
    features = query_weight.shape[1]
    groups, shards = lax.axis_size("pair"), lax.axis_size("mp")
    width = model_width // shards
    rows = pair_count * slot_count
    hidden_units = up_weight.shape[1]
    current_rows = current.transpose(1, 0, 2)
    past_rows = past_tokens.transpose(1, 0, 2)

    def part(fn, *static):
        return lambda *refs: fn(*static, *refs)

    *entries, shifts = call(
        part(pack_kernel, groups),
        [*[struct((key_count, width))] * groups, struct((pair_count, 128), F32)],
        [partners, past_rows],
        flops=rows * width,
        scratch=[
            pltpu.SMEM(partners.shape, jnp.int32),
            pltpu.VMEM((key_count, pair_count, width), BF16),
            pltpu.VMEM((pair_count, key_count, width), BF16),
            pltpu.SemaphoreType.DMA((2,)),
        ],
        specs=[HBM, HBM],
        limit=63 << 20,
    )
    incoming = exchange(entries)
    output_weights = gather(output_weight)
    staged = [key_weight, value_weight, output_weight, incoming[0], shifts]
    key_weight, value_weight, output_weights[0], incoming[0], shifts = call(
        stage_kernel, [struct(a.shape, a.dtype) for a in staged], staged, flops=rows * width
    )
    (queries,) = call(
        query_kernel,
        [struct((pair_count, slot_count, features))],
        [current_rows, query_weight],
        flops=2 * rows * model_width * features,
    )
    away, near = range(shards - 1, shards // 2 - 1, -1), range(shards // 2 - 1, -1, -1)
    block = struct((slot_count, width))
    wide = struct((slot_count, width), F32)

    def narrow(part_of):
        stride, alone = 1, []
        while stride < shards // 2:
            for k in [k for k in part_of if k & stride]:
                received = swap(part_of.pop(k), stride)
                if k ^ stride:
                    (part_of[k ^ stride],) = call(
                        add_kernel,
                        [block],
                        [part_of[k ^ stride], received],
                        flops=slot_count * width,
                    )
                else:
                    alone.append(received)
            stride *= 2
        return alone

    context, attended, terms = [], [], []
    wanted = call(
        part(select_kernel, groups),
        [struct((key_count, width))] * pair_count,
        [shifts, *incoming],
        flops=rows * width,
    )
    for p in range(pair_count):
        context.append(gather(wanted[p]))
    for p in range(pair_count):
        (done,) = call(
            part(attend_kernel, shards, p),
            [struct((slot_count, features))],
            [queries, key_weight, value_weight, *context[p]],
            flops=4 * rows // pair_count * model_width * features,
        )
        attended.append(gather(done))
    for p in range(pair_count):
        (early,) = call(
            part(early_kernel, p),
            [struct((slot_count, model_width), F32)],
            [current_rows, *attended[p][:-1], *output_weights[:-1]],
            flops=2 * slot_count * model_width * features * (shards - 1),
        )
        expanded, share, *sums = call(
            part(mixer_kernel, away),
            [struct((slot_count, hidden_units)), wide, *[block] * len(away)],
            [early, attended[p][-1], output_weights[-1], up_weight, down_weight],
            flops=4 * slot_count * model_width * hidden_units,
            scratch=[pltpu.VMEM((slot_count, model_width), F32)],
            limit=24 << 20,
        )
        far = dict(zip(away, sums))
        narrow(far)
        crossed = swap(far[shards // 2], shards // 2)
        close = dict(
            zip(
                near,
                call(
                    part(near_kernel, near),
                    [*[block] * (len(near) - 1), wide],
                    [expanded, share, down_weight],
                    flops=slot_count * model_width * hidden_units,
                ),
            )
        )
        base = close.pop(0)
        terms += [base, *narrow(close), crossed]
    (result,) = call(
        part(final_kernel, pair_count),
        [struct((slot_count, pair_count, width))],
        [counts, *terms],
        flops=rows * width,
        scratch=[pltpu.VMEM((width // 128, rows, 128), F32)],
    )
    return result.transpose(1, 0, 2)


def solution(mesh):
    placed = (
        P("pair", None, None),
        P("pair", None, None),
        P("pair"),
        P(),
        P(None, "mp"),
        P(None, "mp"),
        P(None, "mp"),
        P("mp", None),
        P(None, "mp"),
        P("mp", None),
    )

    return jax.shard_map(
        body, mesh=mesh, in_specs=placed, out_specs=P("pair", None, "mp"), check_vma=False
    )
```

```python
import jax
import jax.numpy as jnp
from jax import lax
from jax.experimental import pallas as pl
from jax.experimental.pallas import tpu as pltpu
from jax.sharding import PartitionSpec as P


HEAD_DIM = 64
F32, BF16 = jnp.float32, jnp.bfloat16
VMEM = pl.BlockSpec(memory_space=pltpu.VMEM)
SMEM = pl.BlockSpec(memory_space=pltpu.SMEM)
HBM = pl.BlockSpec(memory_space=pltpu.HBM)


def layer_norm(values):
    center = values - jnp.mean(values, axis=-1, keepdims=True)
    spread = jnp.mean(center * center, axis=-1, keepdims=True)
    return center * lax.rsqrt(spread + 1e-06)


def erf_gelu(v):
    return 0.5 * v * (1.0 + lax.erf(v * (0.5**0.5)))


def mm(a, b):
    return jnp.dot(a, b, preferred_element_type=F32)


def call(kernel, outs, ins, flops, limit=16 << 20, scratch=(), specs=None):
    specs = specs or [SMEM if a.dtype == jnp.int32 else VMEM for a in ins]
    moved = sum(a.size * a.dtype.itemsize for a in list(ins) + list(outs))
    return pl.pallas_call(
        kernel,
        out_shape=list(outs),
        in_specs=specs,
        out_specs=[VMEM] * len(outs),
        scratch_shapes=list(scratch),
        cost_estimate=pl.CostEstimate(flops=flops, bytes_accessed=moved, transcendentals=0),
        compiler_params=pltpu.CompilerParams(vmem_limit_bytes=limit),
    )(*ins)


def struct(shape, dtype=BF16):
    return jax.ShapeDtypeStruct(shape, dtype)


def wrap(index, size):
    return jnp.where(index >= size, index - size, index)


def source_slot(partners, dest, mine, pair_count):
    slot = 0
    for j in range(pair_count):
        near = partners[dest * pair_count + j] - mine * pair_count
        slot = jnp.where((near >= 0) & (near < pair_count), near, slot)
    return slot


def pack_kernel(groups, partners_hbm, past, *refs):
    outs, shifts = refs[:groups], refs[groups]
    partners, rows, halves, sems = refs[groups + 1 :]
    pair_count = past.shape[1]
    width = outs[0].shape[-1]
    mine = lax.axis_index("pair")
    start = pl.multiple_of(lax.axis_index("mp") * width, width)
    table = pltpu.make_async_copy(partners_hbm, partners, sems.at[0])
    block = pltpu.make_async_copy(past.at[:, :, pl.ds(start, width)], rows, sems.at[1])
    block.start()
    table.start()
    table.wait()
    slots = [source_slot(partners, wrap(mine + k, groups), mine, pair_count) for k in range(groups)]
    for p in range(pair_count):
        wanted, shift = partners[mine * pair_count + p], 0
        for k in range(1, groups):
            near = wanted - wrap(mine + groups - k, groups) * pair_count
            shift = jnp.where((near >= 0) & (near < pair_count), k, shift)
        shifts[pl.ds(p, 1), :] = jnp.full((1, shifts.shape[1]), shift, jnp.int32).astype(F32)
    block.wait()
    for p in range(pair_count):
        halves[p] = rows[:, p, :].astype(F32).astype(BF16)
    for k in range(groups):
        outs[k][...] = halves[slots[k]]


def own_pair(rows):
    first, second = rows[:, 0, :].astype(F32), rows[:, 1, :].astype(F32)
    return jnp.where(lax.axis_index("mp") % 2 == 0, first, second)


def query_kernel(current, *refs):
    count = len(refs) // 2
    normed = layer_norm(own_pair(current)).astype(BF16)
    for weight, queries in zip(refs[:count], refs[count:]):
        queries[...] = mm(normed, weight[...]).astype(BF16)


def stage_kernel(*refs):
    held = len(refs) // 2
    for source, kept in zip(refs[:held], refs[held:]):
        kept[...] = source[...]


def select_kernel(groups, shifts, *refs):
    incoming, outs = refs[:groups], refs[groups:]
    low = lax.axis_index("mp") % 2
    for j, out in enumerate(outs):
        shift = jnp.max(shifts[pl.ds(low if j == 0 else 1 - low, 1), :])
        for k in range(groups):

            @pl.when(shift == float(k))
            def _():
                out[...] = incoming[k][...]


def normalize(context, outs):
    scale = 1.0 / sum(block.shape[-1] for block in context)
    blocks = [block[...].astype(F32) for block in context]
    mean = sum(jnp.sum(v, axis=-1, keepdims=True) for v in blocks) * scale
    blocks = [v - mean for v in blocks]
    spread = sum(jnp.sum(v * v, axis=-1, keepdims=True) for v in blocks) * scale
    factor = lax.rsqrt(spread + 1e-06)
    for v, out in zip(blocks, outs):
        out[...] = (v * factor).astype(BF16)


def attention(shards, normed, asked, key_weight, value_weight):
    slot_count, features = asked.shape
    width = normed[0].shape[-1]
    me = lax.axis_index("mp")
    lane_head = lax.broadcasted_iota(jnp.int32, (1, features), 1) // HEAD_DIM
    keys = values = 0.0
    for k in range(shards):
        rows = pl.ds(pl.multiple_of((me ^ k) * width, width), width)
        keys += mm(normed[k][...], key_weight[rows, :])
        values += mm(normed[k][...], value_weight[rows, :])
    keys, values = keys.astype(BF16), values.astype(BF16)
    total = jnp.zeros((slot_count, features), F32)
    for h in range(features // HEAD_DIM):
        mask = lane_head == h
        scores = lax.dot_general(
            jnp.where(mask, asked, jnp.zeros_like(asked)),
            keys,
            (((1,), (1,)), ((), ())),
            preferred_element_type=F32,
        )
        scores = scores * HEAD_DIM ** (-0.5)
        lifted = jnp.exp(scores - jnp.max(scores, axis=-1, keepdims=True))
        weights = lifted * (1.0 / jnp.sum(lifted, axis=-1, keepdims=True))
        total = jnp.where(mask, mm(weights.astype(BF16), values), total)
    return total.astype(BF16)


def attend_first(shards, queries, key_weight, value_weight, *refs):
    context, out, normed = refs[:shards], refs[shards], refs[shards + 1 :]
    normalize(context, normed)
    out[...] = attention(shards, normed, queries[...], key_weight, value_weight)


def attend_second(shards, queries, key_weight, value_weight, *refs):
    refs[shards][...] = attention(shards, refs[:shards], queries[...], key_weight, value_weight)


def columns(k, width):
    return pl.ds(pl.multiple_of((lax.axis_index("mp") ^ k) * width, width), width)


def early_kernel(current, *refs):
    count = (len(refs) - 1) // 2
    hidden = own_pair(current)
    for attended, weight in zip(refs[:count], refs[count:-1]):
        hidden += mm(attended[...], weight[...])
    refs[-1][...] = hidden


def mixer_kernel(far, early, *refs):
    late, (ups, downs) = refs[:4], (refs[4:6], refs[6:8])
    hidden_out, first, second, sent = refs[8:]
    hidden = early[...]
    for attended, weight in zip(late[:2], late[2:]):
        hidden += mm(attended[...], weight[...])
    hidden_out[...] = hidden
    mixer_in = layer_norm(hidden).astype(BF16)
    for up, expanded in zip(ups, (first, second)):
        expanded[...] = erf_gelu(mm(mixer_in, up[...])).astype(BF16)
    width = sent.shape[-1]
    total = mm(first[...], downs[0][:, columns(far, width)])
    sent[...] = (total + mm(second[...], downs[1][:, columns(far, width)])).astype(BF16)


def part_kernel(far, first, second, down, other_down, sent):
    width = sent.shape[-1]
    total = mm(first[...], down[:, columns(far, width)])
    sent[...] = (total + mm(second[...], other_down[:, columns(far, width)])).astype(BF16)


def near_kernel(hidden, first, second, down, other_down, *outs):
    width = outs[0].shape[-1]
    for k, out in enumerate(outs):
        total = hidden[:, columns(k, width)] + mm(first[...], down[:, columns(k, width)])
        out[...] = total + mm(second[...], other_down[:, columns(k, width)])


def close_kernel(base, crossed, out):
    out[...] = (base[...] + crossed[...].astype(F32)).astype(BF16)


def final_kernel(counts, base, crossed, other, out, hold):
    slot_count, pair_count, width = out.shape
    lanes = hold.shape[-1]
    low = lax.axis_index("mp") % 2
    slots = lax.broadcasted_iota(jnp.int32, (slot_count, 1), 0)
    mine = base[...] + crossed[...].astype(F32)
    theirs = other[...].astype(F32)
    for p in range(pair_count):
        total = jnp.where(low == p, mine, theirs)
        total = jnp.where(slots < counts[p], total, 0.0)
        for j in range(width // lanes):
            hold[j, pl.ds(p, slot_count, stride=pair_count), :] = total[:, j * lanes : (j + 1) * lanes]
    for j in range(width // lanes):
        tile = hold[j].reshape(slot_count, pair_count, lanes).astype(BF16)
        out[:, :, j * lanes : (j + 1) * lanes] = tile


def swap(value, stride):
    size = lax.axis_size("mp")
    return lax.ppermute(value, "mp", [(i, i ^ stride) for i in range(size)])


def gather(block):
    size = lax.axis_size("mp")
    blocks, stride = {0: block}, size // 2
    while stride:
        blocks |= {k ^ stride: swap(v, stride) for k, v in blocks.items()}
        stride //= 2
    return [blocks[k] for k in range(size)]


def exchange(entries):
    groups = lax.axis_size("pair")
    if groups <= 8:
        moved = [entries[0]]
        for k in range(1, groups):
            ring = [(i, (i + k) % groups) for i in range(groups)]
            moved.append(lax.ppermute(entries[k], "pair", ring))
        return moved
    mine = lax.axis_index("pair")
    order = (jnp.arange(groups) - mine) % groups
    moved = lax.all_to_all(jnp.stack(entries)[order], "pair", 0, 0, tiled=True)
    moved = moved[(mine - jnp.arange(groups)) % groups]
    return [moved[k] for k in range(groups)]


def body(
    current,
    past_tokens,
    counts,
    partners,
    query_weight,
    key_weight,
    value_weight,
    output_weight,
    up_weight,
    down_weight,
):
    pair_count, slot_count, model_width = current.shape
    key_count = past_tokens.shape[1]
    features = query_weight.shape[1]
    groups, shards = lax.axis_size("pair"), lax.axis_size("mp")
    width = model_width // shards
    rows = pair_count * slot_count
    hidden_units = up_weight.shape[1]
    current_rows = current.transpose(1, 0, 2)
    past_rows = past_tokens.transpose(1, 0, 2)

    def part(fn, *static):
        return lambda *refs: fn(*static, *refs)

    *entries, shifts = call(
        part(pack_kernel, groups),
        [*[struct((key_count, width))] * groups, struct((pair_count, 128), F32)],
        [partners, past_rows],
        flops=rows * width,
        scratch=[
            pltpu.SMEM(partners.shape, jnp.int32),
            pltpu.VMEM((key_count, pair_count, width), BF16),
            pltpu.VMEM((pair_count, key_count, width), BF16),
            pltpu.SemaphoreType.DMA((2,)),
        ],
        specs=[HBM, HBM],
        limit=63 << 20,
    )
    incoming = exchange(entries)
    output_weights = gather(output_weight)
    assert pair_count == 2 and shards == 4
    staged = [key_weight, value_weight, output_weight, incoming[0], shifts]
    other_query = swap(query_weight, 1)
    other_key = swap(key_weight, 1)
    other_value = swap(value_weight, 1)
    other_up = swap(up_weight, 1)
    other_down = swap(down_weight, 1)
    key_weight, value_weight, output_weights[0], incoming[0], shifts = call(
        stage_kernel, [struct(a.shape, a.dtype) for a in staged], staged, flops=rows * width
    )
    asked = struct((slot_count, features))
    queries, other_queries = call(
        query_kernel,
        [asked, asked],
        [current_rows, query_weight, other_query],
        flops=2 * rows * model_width * features,
    )
    block = struct((slot_count, width))
    wide = struct((slot_count, width), F32)
    mine, theirs = call(
        part(select_kernel, groups),
        [struct((key_count, width))] * pair_count,
        [shifts, *incoming],
        flops=rows * width,
    )
    beside = swap(theirs, 1)
    context = [mine, beside, swap(mine, 2), swap(beside, 2)]
    attended, *normed = call(
        part(attend_first, shards),
        [asked, *[struct((key_count, width))] * shards],
        [queries, key_weight, value_weight, *context],
        flops=2 * rows * model_width * features,
    )
    (other_attended,) = call(
        part(attend_second, shards),
        [asked],
        [other_queries, other_key, other_value, *normed],
        flops=2 * rows * model_width * features,
    )
    late = [swap(attended, 2), swap(other_attended, 2)]
    (early,) = call(
        early_kernel,
        [struct((slot_count, model_width), F32)],
        [current_rows, attended, other_attended, *output_weights[:2]],
        flops=4 * slot_count * model_width * features,
    )
    downs = [down_weight, other_down]
    hidden, *expanded, part_3 = call(
        part(mixer_kernel, 3),
        [
            struct((slot_count, model_width), F32),
            *[struct((slot_count, hidden_units))] * 2,
            block,
        ],
        [early, *late, *output_weights[2:], up_weight, other_up, *downs],
        flops=5 * slot_count * model_width * hidden_units,
        limit=24 << 20,
    )
    crossed_1 = swap(part_3, 2)
    (part_2,) = call(
        part(part_kernel, 2),
        [block],
        [*expanded, *downs],
        flops=slot_count * model_width * hidden_units,
    )
    crossed_0 = swap(part_2, 2)
    base_0, base_1 = call(
        near_kernel,
        [wide, wide],
        [hidden, *expanded, *downs],
        flops=2 * slot_count * model_width * hidden_units,
    )
    (done,) = call(close_kernel, [block], [base_1, crossed_1], flops=slot_count * width)
    other = swap(done, 1)
    (result,) = call(
        final_kernel,
        [struct((slot_count, pair_count, width))],
        [counts, base_0, crossed_0, other],
        flops=rows * width,
        scratch=[pltpu.VMEM((width // 128, rows, 128), F32)],
    )
    return result.transpose(1, 0, 2)


def solution(mesh):
    placed = (
        P("pair", None, None),
        P("pair", None, None),
        P("pair"),
        P(),
        P(None, "mp"),
        P(None, "mp"),
        P(None, "mp"),
        P("mp", None),
        P(None, "mp"),
        P("mp", None),
    )

    return jax.shard_map(
        body, mesh=mesh, in_specs=placed, out_specs=P("pair", None, "mp"), check_vma=False
    )
```
